128 devices in a mesh: node: 16 (over z, y), dev: 8 (over x, core).
Axes of the slice: x: 4, y: 4, z: 4, core: 2. Of those that a mesh axis runs over, the one named last changes fastest.
Arguments:
- tokens: bfloat16 [8192, 5120], P(('node', 'dev')), may hold values from -6 to 6
- node_ids: int32 [8192, 3], P(('node', 'dev')), may hold values from 0 to 15, all different within a row; in each aligned block of 64 rows (0 to 63, 64 to 127, ...) at most 13 rows name the same one
- expert_pick: int32 [8192, 6], P(('node', 'dev')), may hold values from 0 to 8, all different within a row
- gate_share: bfloat16 [8192, 6], P(('node', 'dev')), may hold values from 0.099609375 to 1
- gate_proj: bfloat16 [48, 1536, 5120], P('node', 'dev'), may hold values from -0.078125 to 0.078125
- up_proj: bfloat16 [48, 1536, 5120], P('node', 'dev'), may hold values from -0.078125 to 0.078125
- down_proj: bfloat16 [48, 1536, 5120], P('node', 'dev'), may hold values from -0.15625 to 0.15625
Outputs:
- moe_out: bfloat16 [8192, 5120], P(('node', 'dev'))
The draws below stay inside these ranges and needn't reach their ends.
Inputs may be any that keep to these rules, and one draw needn't show every extreme that they name: `node_ids`: A token names 3 different groups; at most 13 tokens of one device name one group, and some device reaches 13 in every draw. `expert_pick`: A token names 6 different picks; pick p selects local expert p % 3 of the token's group choice p // 3.
All inputs are finite; a program needn't handle non-finite values.
Results may differ from the reference program's by a relative error of at most 0.0085.
Values may be sent and summed in bfloat16 or wider, within the bound.
No kernel may reach another device: no remote copies, remote signals or barrier semaphores. Data moves between devices by JAX's collectives and lax.ppermute only.
A program may use at most 256 MiB of HBM per device.

```python
import math
import jax
import jax.numpy as jnp
import numpy as np
from jax import lax

D = 5120
FF = 1536
TOP = 6
TOP_NODES = 3
EXP_NODE = 3
TOK_DEV = 64
EXPERTS = 48
CAP = 13
TOKENS = 8192
N_NODE = 16
N_DEV = 8


def level_of(rng, extent, pieces, least, largest):
    def one(axis_at, shards_of):
        steps = jax.random.uniform(jax.random.fold_in(jax.random.fold_in(rng, 6), axis_at), (shards_of,), jnp.float32, least / len(pieces), largest / len(pieces))
        return jnp.repeat(jnp.exp(steps), extent[axis_at] // shards_of).reshape((-1,) + (1,) * (len(extent) - axis_at - 1))

    gain = one(*pieces[0])
    for cut in pieces[1:]:
        gain = gain * one(*cut)
    return gain


def different_ones(own_key, rows, count, top, lift):
    order = jax.random.permutation(jax.random.fold_in(own_key, 1), count)
    pull = order
    for power in range(3):
        pull = pull * pull // count
    pull = pull * lift // count
    lots = jax.random.randint(jax.random.fold_in(own_key, 2), (rows, count), 0, 4096) + pull
    fixed_rows = jax.random.permutation(jax.random.fold_in(own_key, 3), rows)[jnp.arange(count) % rows]
    lots = jnp.where(jnp.arange(rows)[:, None] == fixed_rows[None, :], 1 << 14, lots)
    merit = lots * count + jnp.arange(count)
    return lax.top_k(merit.astype(jnp.int32), top)[1].astype(jnp.int32)


def deal_out(rng, own, number, rows, count, top, bound, lean):
    sequence = jax.random.permutation(rng, count)
    packed, common = portions_of(count, rows * top, bound, lean, True), portions_of(count, rows * top, bound, lean, False)
    places = jnp.arange(count)

    def named(lengths, offset_by):
        used = int((lengths > 0).sum())
        fixed = max(1, used // 4)
        passed = fixed + (places - fixed + offset_by * (used - fixed)) % max(1, count - fixed)
        return jnp.zeros((count,), jnp.int32).at[sequence[jnp.where(places < fixed, places, passed)]].set(jnp.asarray(lengths, jnp.int32))

    lengths = jnp.where(number % 4 == 0, named(packed, number // 4), named(common, number - number // 4 - 1))
    mixed = jax.random.permutation(jax.random.fold_in(own, 3), count)
    donor, receiver = mixed[0:count // 2 * 2:2], mixed[1:count // 2 * 2:2]
    slack = jnp.minimum(lengths[donor] - 1, bound - lengths[receiver]) // 2
    slack = jnp.where((donor == sequence[0]) | (receiver == sequence[0]) | (lengths[receiver] == 0), 0, jnp.maximum(slack, 0))
    passed = jax.random.randint(jax.random.fold_in(own, 4), (count // 2,), 0, 1 << 20) % (slack + 1)
    lengths = lengths.at[donor].add(-passed).at[receiver].add(passed)
    members = jnp.searchsorted(jnp.cumsum(lengths), jnp.arange(rows * top), side="right").astype(jnp.int32)
    table = members.reshape(top, rows).T
    table = table[jax.random.permutation(jax.random.fold_in(own, 1), rows)]
    offset_by = jax.random.randint(jax.random.fold_in(own, 2), (rows, 1), 0, top)
    return jnp.take_along_axis(table, (jnp.arange(top)[None, :] + offset_by) % top, axis=1)


def portions_of(count, total, bound, slope, full):
    loads = [(1 << 20) // math.isqrt(grade ** slope) + 1 for grade in range(1, count + 1)]
    largest = bound if full else min(bound, max(-(-total // count), total * loads[0] // sum(loads)))
    least = 1 if total - largest >= count - 1 else 0
    given, surplus = [largest] + [least] * (count - 1), total - largest - least * (count - 1)
    while surplus > 0:
        free = [i for i in range(1, count) if given[i] < largest] or [i for i in range(1, count) if given[i] < bound]
        whole, left = sum([loads[i] for i in free]), surplus
        for i in free:
            extra = min(bound - given[i], max(1, left * loads[i] // whole), surplus)
            given[i] = given[i] + extra
            surplus = surplus - extra
    return np.array(given)


def noise(key, dims, spread, bound, cuts=(), kind=jnp.bfloat16):
    drawn = jax.random.normal(key, dims, jnp.float32) * spread
    if len(cuts) > 0:
        drawn = level_of(key, dims, cuts, -0.22, 0.18) * drawn
    return jnp.clip(drawn, min=-bound, max=bound).astype(kind)


def setup_inputs(seed: int = 0) -> dict:
    streams_of = jax.random.split(jax.random.key(seed), 8)
    tokens = noise(streams_of[0], (TOKENS, D), 1.0, 6.0, ((0, 128),))
    node_ids_keys = jax.random.split(jax.random.fold_in(streams_of[1], 1), TOKENS // TOK_DEV)
    node_ids_turns = jax.random.permutation(jax.random.fold_in(streams_of[1], 3), TOKENS // TOK_DEV)
    node_ids = jax.vmap(lambda own, number: deal_out(jax.random.fold_in(streams_of[1], 2), own, number, TOK_DEV, N_NODE, TOP_NODES, CAP, 2))(node_ids_keys, node_ids_turns).reshape((TOKENS, TOP_NODES))
    expert_pick = different_ones(streams_of[2], TOKENS, TOP_NODES * EXP_NODE, TOP, 0)
    gate_share = jnp.clip(jnp.exp(math.log(1.0) - 2.306499 * jax.random.uniform(streams_of[3], (TOKENS, TOP), jnp.float32) ** level_of(streams_of[3], (TOKENS, TOP), ((0, 128),), -0.2, 0.2)), 0.099609375, 1.0).astype(jnp.bfloat16)
    gate_proj = noise(streams_of[4], (EXPERTS, FF, D), D ** -0.5, 0.078125, ((0, 16), (1, 8)))
    up_proj = noise(streams_of[5], (EXPERTS, FF, D), D ** -0.5, 0.078125, ((0, 16), (1, 8)))
    down_proj = noise(streams_of[6], (EXPERTS, FF, D), FF ** -0.5, 0.15625, ((0, 16), (1, 8)))
    return {"tokens": tokens, "node_ids": node_ids, "expert_pick": expert_pick, "gate_share": gate_share, "gate_proj": gate_proj, "up_proj": up_proj, "down_proj": down_proj}


def reference(tokens, node_ids, expert_pick, gate_share, gate_proj, up_proj, down_proj):
    token_count = tokens.shape[0]
    capacity = CAP * N_NODE * N_DEV
    candidates = TOP_NODES * EXP_NODE
    slice_width = FF // N_DEV
    picked = (expert_pick[:, :, None] == jnp.arange(candidates, dtype=jnp.int32)[None, None, :]).astype(jnp.float32)
    shares = jnp.einsum('tj,tjq->tq', gate_share.astype(jnp.float32), picked, precision=lax.Precision.HIGHEST)
    shares = shares.reshape(token_count, TOP_NODES, EXP_NODE)
    contract = (((1,), (1,)), ((), ()))

    def per_node(total, node_index):
        hit_mask = (node_ids == node_index).astype(jnp.int32)
        chosen = jnp.sum(hit_mask, axis=1) > 0
        positions = jnp.nonzero(chosen, size=capacity, fill_value=0)[0].astype(jnp.int32)
        is_valid = (jnp.arange(capacity, dtype=jnp.int32) < jnp.sum(chosen.astype(jnp.int32))).astype(jnp.float32)
        node_shares = jnp.einsum('tk,tke->te', hit_mask.astype(jnp.float32), shares, precision=lax.Precision.HIGHEST)
        node_shares = node_shares[positions] * is_valid[:, None]
        tok_rows = tokens[positions]
        accumulated = jnp.zeros((capacity, N_DEV, D), jnp.float32)
        for expert_local in range(EXP_NODE):
            expert = (node_index * EXP_NODE + expert_local).astype(jnp.int32)
            w_gate = lax.dynamic_index_in_dim(gate_proj, expert, 0, keepdims=False)
            w_up = lax.dynamic_index_in_dim(up_proj, expert, 0, keepdims=False)
            w_down = lax.dynamic_index_in_dim(down_proj, expert, 0, keepdims=False)
            gate_val = lax.dot_general(tok_rows, w_gate, contract, preferred_element_type=jnp.float32)
            up_val = lax.dot_general(tok_rows, w_up, contract, preferred_element_type=jnp.float32)
            hidden = (jax.nn.silu(gate_val) * up_val).astype(jnp.bfloat16)
            grouped = jnp.einsum('rgf,gfd->rgd', hidden.reshape(capacity, N_DEV, slice_width).astype(jnp.float32),
                                 w_down.reshape(N_DEV, slice_width, D).astype(jnp.float32),
                                 precision=lax.Precision.HIGHEST)
            accumulated = accumulated + node_shares[:, expert_local, None, None] * grouped
        partial_value = lax.optimization_barrier(accumulated.astype(jnp.bfloat16)).astype(jnp.float32)
        contrib = jnp.sum(partial_value, axis=1) * is_valid[:, None]
        return total.at[positions].add(contrib), None

    total, _ = lax.scan(per_node, jnp.zeros((token_count, D), jnp.float32), jnp.arange(N_NODE, dtype=jnp.int32))
    return total.astype(jnp.bfloat16)
```

```python
import jax
import jax.numpy as jnp
from jax import lax
from jax.experimental import pallas as pl
from jax.experimental.pallas import tpu as pltpu
from jax.sharding import Mesh
from jax.sharding import PartitionSpec as P

NODE = ("z", "y")
ALL = ("z", "y", "x", "c")
CHUNKS = ((0, 8, 64), (8, 13, 48))
PAD = 8
STEP = 1024
BF = jnp.bfloat16
F32 = jnp.float32


UP = [(i, (i + 1) % 4) for i in range(4)]
DOWN = [(i, (i - 1) % 4) for i in range(4)]
SWAP = [(0, 1), (1, 0)]


def mm(a, b, dims=((1,), (0,)), out=F32):
    return lax.dot_general(a, b, (dims, ((), ())), preferred_element_type=F32).astype(out)


def add(*terms):
    total = terms[0].astype(F32)
    for term in terms[1:]:
        total = total + term.astype(F32)
    return total.astype(BF)


def routing(node_ids, node_count):
    tok_count = node_ids.shape[0]
    nodes = jnp.arange(node_count, dtype=jnp.int32)
    choose = (node_ids[:, :, None] == nodes[None, None, :]).astype(F32)
    counts = jnp.sum(choose, axis=1)
    earlier = (jnp.arange(tok_count)[:, None] > jnp.arange(tok_count)[None, :]).astype(F32)
    before = mm(earlier, counts)
    slot = jnp.sum(choose * before[:, None, :], axis=2)
    return slot.astype(jnp.int32)


def one_hot_rows(target, rows):
    ids = jnp.arange(rows, dtype=jnp.int32)[:, None]
    hit = ids == target[None, :, 0]
    for k in range(1, target.shape[1]):
        hit = hit | (ids == target[None, :, k])
    return hit.astype(BF)


def row_weights(target, expert_pick, gate_share, rows, local_count):
    tok_count, choices = target.shape
    picked = (
        expert_pick[:, :, None]
        == jnp.arange(choices * local_count, dtype=jnp.int32)[None, None, :]
    ).astype(F32)
    shares = jnp.sum(gate_share.astype(F32)[:, :, None] * picked, axis=1).astype(BF)
    shares = jnp.pad(
        shares.reshape(tok_count, choices, local_count), ((0, 0), (0, 0), (0, 128 - local_count))
    )
    ids = jnp.arange(rows, dtype=jnp.int32)[:, None]
    total = 0.0
    for k in range(choices):
        total = total + mm((ids == target[None, :, k]).astype(BF), shares[:, k, :])
    return total.astype(BF)


def exchange(rows, node_count):
    width = rows.shape[1]
    got = lax.all_to_all(
        rows.reshape(node_count, -1, width), NODE, split_axis=0, concat_axis=0, tiled=True
    )
    return got.reshape(-1, width)


def hidden_body(*refs):
    pieces, gates = refs[:16], refs[16:32]
    wg, wu, own_out, sib_out, w_ref, acc_ref = refs[32:]
    k = pl.program_id(0)
    joint = wg.shape[0]
    offset = w_ref.shape[0] - joint

    @pl.when(k == 0)
    def _():
        w_ref[...] = jnp.zeros_like(w_ref)
        acc_ref[...] = jnp.zeros_like(acc_ref)

    w_ref[:joint, :] = wg[...]
    w_ref[offset:, :] = wu[...]
    x = jnp.concatenate([p[...] for p in pieces], axis=0)
    acc_ref[...] += lax.dot_general(
        x, w_ref[...], (((1,), (1,)), ((), ())), preferred_element_type=F32
    )

    @pl.when(k == pl.num_programs(0) - 1)
    def _():
        gate = jnp.concatenate([p[...] for p in gates], axis=0).astype(F32)
        lane = lax.broadcasted_iota(jnp.int32, (gate.shape[0], joint), 1)
        third = joint // 3
        weight = jnp.where(
            lane < third, gate[:, 0:1], jnp.where(lane < 2 * third, gate[:, 1:2], gate[:, 2:3])
        )
        g = acc_ref[:, :joint]
        u = acc_ref[:, offset:]
        hid = (g / (1.0 + jnp.exp(-g)) * u * weight).astype(BF)
        half = hid.shape[0] // 2
        own_out[...] = hid[:half]
        sib_out[...] = hid[half:]


def hidden_of(pieces, gate_w, up_w):
    joint, model_width = gate_w.shape
    rows = sum(p.shape[0] for p in pieces)
    wide = -(-joint // 128) * 128 + joint
    specs = [pl.BlockSpec((p.shape[0], STEP), lambda k: (0, k)) for p in pieces]
    specs += [pl.BlockSpec((p.shape[0], 128), lambda k: (0, model_width // 128)) for p in pieces]
    specs += [pl.BlockSpec((joint, STEP), lambda k: (0, k))] * 2
    return pl.pallas_call(
        hidden_body,
        grid=(model_width // STEP,),
        in_specs=specs,
        out_specs=[pl.BlockSpec((rows // 2, joint), lambda k: (0, 0))] * 2,
        out_shape=[jax.ShapeDtypeStruct((rows // 2, joint), BF)] * 2,
        scratch_shapes=[pltpu.VMEM((wide, STEP), BF), pltpu.VMEM((rows, wide), F32)],
        compiler_params=pltpu.CompilerParams(vmem_limit_bytes=40 * 1024 * 1024),
        cost_estimate=pl.CostEstimate(
            flops=2 * rows * wide * model_width, bytes_accessed=30 * 2**20, transcendentals=0
        ),
    )(*pieces, *pieces, gate_w, up_w)


def ring_gather(top, bottom):
    low_top = lax.ppermute(top, "x", UP)
    high_bottom = lax.ppermute(bottom, "x", DOWN)
    low_bottom = lax.ppermute(bottom, "x", UP)
    high_top = lax.ppermute(top, "x", DOWN)
    far_top = lax.ppermute(low_top, "x", UP)
    far_bottom = lax.ppermute(high_bottom, "x", DOWN)
    own = [top, bottom, low_top, low_bottom, high_top, high_bottom, far_top, far_bottom]
    return own + [lax.ppermute(p, "c", SWAP) for p in own]


def ring_reduce(own, sib, down_w, top):
    block = own.shape[0] // 4
    split = 3 * block
    far_away = lax.ppermute(mm(sib[split:], down_w, out=BF), "c", SWAP)
    near_away = lax.ppermute(mm(sib[:split], down_w, out=BF), "c", SWAP)
    far = add(mm(own[split:], down_w), far_away)
    near = add(mm(own[:split], down_w), near_away)
    up_top = lax.ppermute(far[:top], "x", UP)
    down_bottom = lax.ppermute(far[top:], "x", DOWN)
    here, low, high = near[:block], near[block : 2 * block], near[2 * block :]
    low_bottom = lax.ppermute(high[top:], "x", UP)
    high_top = lax.ppermute(low[:top], "x", DOWN)
    low_top = lax.ppermute(add(high[:top], up_top), "x", UP)
    high_bottom = lax.ppermute(add(low[top:], down_bottom), "x", DOWN)
    return add(here[:top], low_top, high_top), add(here[top:], low_bottom, high_bottom)


def shards(tokens, node_ids, expert_pick, gate_share, gate_proj, up_proj, down_proj):
    model_width = tokens.shape[1]
    node_count = 16
    local_count, hidden_width, _ = gate_proj.shape
    joint = local_count * hidden_width
    gate_w = gate_proj.reshape(joint, model_width)
    up_w = up_proj.reshape(joint, model_width)
    down_w = down_proj.reshape(joint, model_width)
    rows = node_count * PAD

    slot = routing(node_ids, node_count)
    selectors, compacts, hidden = [], [], []
    for first, end, top in CHUNKS:
        inside = (slot >= first) & (slot < end)
        target = jnp.where(inside, node_ids * PAD + slot - first, -1)
        selector = one_hot_rows(target, rows)
        weights = row_weights(target, expert_pick, gate_share, rows, local_count)
        send = jnp.concatenate([mm(selector, tokens, out=BF), weights], axis=1)
        got = exchange(send, node_count)
        used = end - first
        compact = None
        if used == PAD:
            halves = got[:top], got[top:]
        else:
            ids = jnp.arange(node_count * used, dtype=jnp.int32)
            place = ids // used * PAD + ids % used
            compact = (place[:, None] == jnp.arange(rows, dtype=jnp.int32)[None, :]).astype(BF)
            halves = mm(compact[:top], got, out=BF), mm(compact[top:], got, out=BF)
        hidden.append(hidden_of(ring_gather(*halves), gate_w, up_w))
        selectors.append(selector)
        compacts.append(compact)

    out = 0.0
    for (first, end, top), (own, sib), selector, compact in zip(
        CHUNKS, hidden, selectors, compacts
    ):
        upper, lower = ring_reduce(own, sib, down_w, top)
        if compact is None:
            total = jnp.concatenate([upper, lower], axis=0)
        else:
            total = mm(compact[:top], upper, ((0,), (0,))) + mm(
                compact[top:], lower, ((0,), (0,))
            )
            total = total.astype(BF)
        out = out + mm(selector, exchange(total, node_count), ((0,), (0,)))
    return out.astype(BF)


def solution(mesh):
    split = Mesh(mesh.devices.reshape(4, 4, 4, 2), ALL)
    row = P(ALL, None)
    weight = P(NODE, ("x", "c"), None)
    return jax.shard_map(
        shards,
        mesh=split,
        in_specs=(row, row, row, row, weight, weight, weight),
        out_specs=row,
        check_vma=False,
    )
```
